32 devices in a mesh: res: 4 (over x, core), blk: 8 (over z, y).
Axes of the slice: x: 2, y: 2, z: 4, core: 2. Of those that a mesh axis runs over, the one named last changes fastest.
Arguments:
- modes: float32 [2, 8, 4194304], P(None, 'res', 'blk'), may hold values from -0.078125 to 0.078125
Outputs:
- product_modes: float32 [2, 8, 4194304], P(None, 'res', 'blk')
The draws below stay inside these ranges and needn't reach their ends.
All inputs are finite; a program needn't handle non-finite values.
Results may differ from the reference program's by a relative error of at most 0.000098.
Values sent between devices are 32-bit elements; how exact they have to be, the bound alone decides.
A program may use at most 192 MiB of HBM per device.

```python
import jax
import jax.numpy as jnp

MODES = 33554432
EIGHTH = 4194304
PADDED = 50331648


def block_levels(key, extent, cuts, smallest, largest):
    gain, own = 1.0, jax.random.fold_in(key, 6)
    for dim, blocks in cuts:
        heights = jnp.exp(jax.random.uniform(jax.random.fold_in(own, dim), (blocks,), jnp.float32, smallest / len(cuts), largest / len(cuts)))
        gain = gain * jnp.repeat(heights, extent[dim] // blocks).reshape([-1 if axis == dim else 1 for axis in range(len(extent))])
    return gain


def gaussian(own_key, dims, scale, most, shards=(), dtype=jnp.bfloat16):
    loudness = block_levels(own_key, dims, shards, -0.22, 0.18) if shards else 1.0
    values = jax.random.normal(own_key, dims, jnp.float32) * scale * loudness
    return jnp.minimum(jnp.maximum(values, -most), most).astype(dtype)


def setup_inputs(seed: int = 0) -> dict:
    key_of = jax.random.split(jax.random.key(seed), 2)
    modes = gaussian(key_of[0], (2, 8, EIGHTH), (MODES ** -0.25), 0.078125, ((1, 4), (2, 8)), jnp.float32)
    return {"modes": modes}


def reference(modes):
    series = (modes[0] + 1j * modes[1]).reshape(MODES)
    padded = jnp.pad(series, (0, PADDED - MODES))
    physical = jnp.fft.ifft(padded) * PADDED
    spectrum = jnp.fft.fft(physical * physical) / PADDED
    kept = spectrum[MODES // 2: MODES // 2 + MODES]
    result = jnp.stack([jnp.real(kept), jnp.imag(kept)]).reshape(2, 8, EIGHTH)
    return result.astype(jnp.float32)
```

```python
import functools
import math

import jax
import jax.numpy as jnp
import ml_dtypes
import numpy as np
from jax import lax
from jax.experimental import pallas as pl
from jax.experimental.pallas import tpu as pltpu
from jax.sharding import PartitionSpec as P

AXES = ("res", "blk")
ROWS = 8
UNITS = 4
TILE = 256
VMEM = 60 * 1024 * 1024


def split(value):
    high = value.astype(jnp.bfloat16)
    return high, (value - high.astype(jnp.float32)).astype(jnp.bfloat16)


def host_split(table):
    high = table.astype(ml_dtypes.bfloat16)
    return np.stack([high, (table - high.astype(np.float64)).astype(ml_dtypes.bfloat16)])


def host_turn(left, right, period):
    angle = 2.0 * math.pi / period * ((left[:, None] * right[None, :]) % period)
    return np.cos(angle), np.sin(angle)


def dot(left, right):
    return jnp.dot(left, right, preferred_element_type=jnp.float32)


def dot3(left, right):
    return dot(left[0], right[0]) + dot(left[1], right[0]) + dot(left[0], right[1])


def columns(ref, part, first, lanes, own, high):
    stride = ref.shape[1] // high
    starts = [(first + i) * own + pl.program_id(1) for i in range(lanes)]
    return [(part, pl.ds(start, high, stride=stride)) for start in starts]


def forward_kernel(tile, own, x_ref, m_ref, w_ref, t_ref, o_ref, l_ref):
    high, low = m_ref.shape[3], t_ref.shape[3]
    rows = m_ref.shape[2] // 2
    lanes = tile // 128

    def first(j, _):
        at = pl.ds(pl.multiple_of(j * tile, tile), tile)
        m = (m_ref[0, 0], m_ref[0, 1])
        real, imag = [
            dot3(m, split(jnp.concatenate(
                [x_ref[p, r, :] for p, r in columns(x_ref, part, j * lanes, lanes, own, high)], axis=1
            )))
            for part in range(2)
        ]
        re, im = real[:rows] - imag[rows:], imag[:rows] + real[rows:]
        cos, sin = w_ref[0, 0, :, at], w_ref[0, 1, :, at]
        l_ref[0, :rows, at], l_ref[1, :rows, at] = split(re * cos - im * sin)
        l_ref[0, rows:, at], l_ref[1, rows:, at] = split(re * sin + im * cos)
        return 0

    def second(j, _):
        at = pl.ds(pl.multiple_of(j * tile, tile), tile)
        value = (l_ref[0], l_ref[1])
        by_cos = dot3(value, (t_ref[0, 0, :, at], t_ref[0, 1, :, at]))
        by_sin = dot3(value, (t_ref[1, 0, :, at], t_ref[1, 1, :, at]))
        shape = (rows // ROWS, ROWS, tile)
        o_ref[:, 0, 0, :, at] = (by_cos[:rows] - by_sin[rows:]).reshape(shape)
        o_ref[:, 0, 1, :, at] = (by_sin[:rows] + by_cos[rows:]).reshape(shape)
        return 0

    lax.fori_loop(0, low // tile, first, 0)
    lax.fori_loop(0, low // tile, second, 0)


def inverse_kernel(tile, own, units, x_ref, m_ref, w_ref, t_ref, *rest):
    a_ref, o_ref, l_ref = rest if len(rest) == 3 else (None, *rest)
    high, low = m_ref.shape[2], t_ref.shape[3]
    rows = x_ref.shape[0] * ROWS
    lanes = tile // 128
    for part in range(2):
        value = split(x_ref[:, 0, part].reshape(rows, low))
        l_ref[0, part * rows:(part + 1) * rows], l_ref[1, part * rows:(part + 1) * rows] = value

    def column(j, _):
        at = pl.ds(pl.multiple_of(j * tile, tile), tile)
        value = (l_ref[0], l_ref[1])
        by_cos = dot3(value, (t_ref[0, 0, :, at], t_ref[0, 1, :, at]))
        by_sin = dot3(value, (t_ref[1, 0, :, at], t_ref[1, 1, :, at]))
        re, im = by_cos[:rows] + by_sin[rows:], by_cos[rows:] - by_sin[:rows]
        cos, sin = w_ref[0, 0, :, at], w_ref[0, 1, :, at]
        re, im = re * cos + im * sin, im * cos - re * sin
        m = (m_ref[0, 0], m_ref[0, 1])
        real = dot3(m, split(jnp.concatenate([re, im], axis=0)))
        imag = dot3(m, split(jnp.concatenate([im, -re], axis=0)))
        for part, value in enumerate((real, imag)):
            for i, (p, r) in enumerate(columns(o_ref, part, j * lanes, lanes, own, high)):
                now = value[:, i * 128:(i + 1) * 128]
                before = 0.0 if a_ref is None else a_ref[p, r, :]
                if units > 1:
                    before = jnp.where(pl.program_id(0) == 0, before, o_ref[p, r, :])
                o_ref[p, r, :] = now + before
        return 0

    lax.fori_loop(0, low // tile, column, 0)


def rotate(value, step, period, scale=1.0):
    re, im = value
    step %= period
    if (4 * step) % period == 0:
        turns = (4 * step) // period
        re, im = [(re, im), (-im, re), (-re, -im), (im, -re)][turns]
        return (re, im) if scale == 1.0 else (re * scale, im * scale)
    angle = 2.0 * math.pi * step / period
    cos, sin = math.cos(angle) * scale, math.sin(angle) * scale
    if (8 * step) % period == 0:
        root = math.sqrt(0.5) * scale
        plus, minus = (re + im) * root, (re - im) * root
        return {1: (minus, plus), 3: (-plus, minus), 5: (-minus, -plus), 7: (plus, -minus)}[(8 * step) // period]
    return re * cos - im * sin, re * sin + im * cos


def add(a, b):
    return a[0] + b[0], a[1] + b[1]


def sub(a, b):
    return a[0] - b[0], a[1] - b[1]


def small_dft(values, sign):
    n = len(values)
    if n == 1:
        return values
    if n % 4:
        return [add(values[0], values[1]), sub(values[0], values[1])]
    q = n // 4
    parts = [[], [], [], []]
    for i in range(q):
        a, b, c, d = values[i], values[i + q], values[i + 2 * q], values[i + 3 * q]
        s, t, u, v = add(a, c), sub(a, c), add(b, d), rotate(sub(b, d), sign, 4)
        parts[0].append(add(s, u))
        parts[1].append(rotate(add(t, v), sign * i, n))
        parts[2].append(rotate(sub(s, u), 2 * sign * i, n))
        parts[3].append(rotate(sub(t, v), 3 * sign * i, n))
    done = [small_dft(part, sign) for part in parts]
    return [done[i % 4][i // 4] for i in range(n)]


def square_kernel(blocks, start, scale, x_ref, o_ref):
    sign = (1 - 2 * ((start + pl.program_id(0)) % 2)).astype(jnp.float32)
    owners, own = x_ref.shape[:2]
    count = owners * own
    half = count // 2
    period = 3 * half

    def place(q):
        eighth, block = divmod(q, blocks)
        return (eighth // own) * blocks + block, eighth % own

    def load(q):
        owner, e = place(q)
        return x_ref[owner, e, 0], x_ref[owner, e, 1]

    third = []
    for rho in range(3):
        folded = [
            rotate(add(load(q), rotate(load(q + half), rho, 3)), rho * q, period) for q in range(half)
        ]
        values = small_dft(folded, 1)
        values = [(re * re - im * im, 2.0 * (re * im)) for re, im in values]
        values = small_dft(values, -1)
        third.append([rotate(value, -rho * q, period) for q, value in enumerate(values)])

    def coefficient(c):
        q, s = c % half, c // half
        total = third[0][q]
        for rho in (1, 2):
            total = add(total, rotate(third[rho][q], -rho * s, 3))
        return total

    before = coefficient(half - 1)
    for c in range(half, 3 * half):
        now = coefficient(c)
        both = now[0] + sign * before[0], now[1] + sign * before[1]
        owner, e = place(c - half)
        o_ref[owner, e, 0] = both[0] * scale
        o_ref[owner, e, 1] = both[1] * scale
        before = now


def on_device(modes):
    own, width = modes.shape[1:]
    blocks = lax.axis_size("blk")
    devices = blocks * lax.axis_size("res")
    units = UNITS
    while units > 2 and width // (devices * ROWS * units // 2) < 128:
        units //= 2
    rows = devices * ROWS
    high = rows * units // 2
    low = width // high
    tile = min(TILE, low)

    highs, lows = np.arange(high), np.arange(low)
    low_tables = np.stack([host_split(table) for table in host_turn(lows, lows, low)])
    twiddles, befores, afters = [], [], []
    for unit in range(units):
        freq = 2 * (unit // 2 * rows + np.arange(rows)) + unit % 2
        twiddles.append(np.stack(host_turn(freq, lows, 2 * width)).astype(np.float32))
        cos, sin = host_turn(freq, highs, 2 * high)
        befores.append(host_split(np.concatenate([cos, sin], axis=0)))
        afters.append(host_split(np.concatenate([cos.T, sin.T], axis=1)))
    low_tables, twiddles, befores, afters = [
        jnp.asarray(a) for a in (low_tables, np.stack(twiddles), np.stack(befores), np.stack(afters))
    ]

    once = pl.Buffered(1)
    tables = pl.BlockSpec(low_tables.shape, lambda u, e: (0, 0, 0, 0), pipeline_mode=once)
    field = (2, own * width // 128, 128)
    fields = pl.BlockSpec(field, lambda u, e: (0, 0, 0), pipeline_mode=once)
    packet = pl.BlockSpec((devices, 1, 2, ROWS, low), lambda u, e: (0, e, 0, u, 0))
    params = pltpu.CompilerParams(vmem_limit_bytes=VMEM)
    scratch = [pltpu.VMEM((2, 2 * rows, low), jnp.bfloat16)]

    def of_unit(start, table):
        return pl.BlockSpec((1, *table.shape[1:]), lambda u, e: (start + u, 0, 0, 0))

    def message(count):
        return jax.ShapeDtypeStruct((devices, own, 2, count * ROWS, low), jnp.float32)

    def cost(count):
        flops = count * own * 3 * 8 * rows * low * (high + low)
        return pl.CostEstimate(flops=flops, bytes_accessed=8 * own * width, transcendentals=0)

    def forward(start, count, field_in):
        return pl.pallas_call(
            functools.partial(forward_kernel, tile, own),
            out_shape=message(count),
            grid=(count, own),
            in_specs=[fields, of_unit(start, befores), of_unit(start, twiddles), tables],
            out_specs=packet,
            scratch_shapes=scratch,
            compiler_params=params,
            cost_estimate=cost(count),
            name="forward",
        )(field_in, befores, twiddles, low_tables)

    def inverse(start, count, packets, total):
        extra = [] if total is None else [total]
        return pl.pallas_call(
            functools.partial(inverse_kernel, tile, own, count),
            out_shape=jax.ShapeDtypeStruct(field, jnp.float32),
            grid=(count, own),
            in_specs=[packet, of_unit(start, afters), of_unit(start, twiddles), tables, *([fields] * len(extra))],
            out_specs=pl.BlockSpec(field, lambda u, e: (0, 0, 0)),
            scratch_shapes=scratch,
            compiler_params=params,
            cost_estimate=cost(count),
            name="inverse",
        )(packets, afters, twiddles, low_tables, *extra)

    def square(start, offset, count, packets):
        def lanes(skip):
            return pl.BlockSpec((devices, own, 2, ROWS, 128), lambda u, j: (0, 0, 0, skip + u, j))

        scale = 1.0 / (3 * devices * own * width)
        return pl.pallas_call(
            functools.partial(square_kernel, blocks, start + offset, scale),
            out_shape=message(count),
            grid=(count, low // 128),
            in_specs=[lanes(offset)],
            out_specs=lanes(0),
            compiler_params=params,
            cost_estimate=cost(count),
            name="square",
        )(packets)

    def exchange(packets):
        return lax.all_to_all(packets, AXES, split_axis=0, concat_axis=0, tiled=True)

    field_in = modes.reshape(2, own, width // 128, 128).transpose(0, 2, 1, 3).reshape(field)
    rest = units - 1
    first = exchange(forward(0, 1, field_in))
    second = exchange(forward(1, rest, field_in))
    home = exchange(square(0, 0, 1, first))
    if rest > 1:
        middle = exchange(square(1, 0, rest - 1, second))
    last = square(1, rest - 1, 1, second)
    total = inverse(0, 1, home, None)
    last, total = lax.optimization_barrier((last, total))
    last = exchange(last)
    if rest > 1:
        total = inverse(1, rest - 1, middle, total)
    total = inverse(rest, 1, last, total)
    total = total.reshape(2, width // 128, own, 128).transpose(0, 2, 1, 3)
    return total.reshape(2, own, width)


def solution(mesh):
    return jax.shard_map(
        on_device,
        mesh=mesh,
        in_specs=(P(None, "res", "blk"),),
        out_specs=P(None, "res", "blk"),
        check_vma=False,
    )
```

```python
import functools
import math

import jax
import jax.numpy as jnp
import ml_dtypes
import numpy as np
from jax import lax
from jax.experimental import pallas as pl
from jax.experimental.pallas import tpu as pltpu
from jax.sharding import PartitionSpec as P

AXES = ("res", "blk")
ROWS = 8
UNITS = 8
TILE = 512
VMEM = 60 * 1024 * 1024


def split(value):
    high = value.astype(jnp.bfloat16)
    return high, (value - high.astype(jnp.float32)).astype(jnp.bfloat16)


def host_split(table):
    high = table.astype(ml_dtypes.bfloat16)
    return np.stack([high, (table - high.astype(np.float64)).astype(ml_dtypes.bfloat16)])


def host_turn(left, right, period):
    angle = 2.0 * math.pi / period * ((left[:, None] * right[None, :]) % period)
    return np.cos(angle), np.sin(angle)


def dot(left, right):
    return jnp.dot(left, right, preferred_element_type=jnp.float32)


def dot3(left, right):
    return dot(left[0], right[0]) + dot(left[1], right[0]) + dot(left[0], right[1])


def columns(ref, part, first, lanes, own, high):
    stride = ref.shape[1] // high
    starts = [(first + i) * own + pl.program_id(0) for i in range(lanes)]
    return [(part, pl.ds(start, high, stride=stride)) for start in starts]


def forward_kernel(tile, own, x_ref, m_ref, w_ref, t_ref, o_ref, f_ref, l_ref):
    high, low = m_ref.shape[3], t_ref.shape[3]
    rows = m_ref.shape[2] // 2
    lanes = tile // 128

    def column(j):
        return pl.ds(pl.multiple_of(j * tile, tile), tile)

    @pl.when(pl.program_id(1) == 0)
    def _():
        def field(j, _):
            for part in range(2):
                for i, (p, r) in enumerate(columns(x_ref, part, j * lanes, lanes, own, high)):
                    at = pl.ds(pl.multiple_of(j * tile, tile) + i * 128, 128)
                    f_ref[0, part, :, at], f_ref[1, part, :, at] = split(x_ref[p, r, :])
            return 0

        lax.fori_loop(0, low // tile, field, 0)

    def first(j, _):
        at = column(j)
        m = (m_ref[0, 0], m_ref[0, 1])
        real = dot3(m, (f_ref[0, 0, :, at], f_ref[1, 0, :, at]))
        imag = dot3(m, (f_ref[0, 1, :, at], f_ref[1, 1, :, at]))
        re, im = real[:rows] - imag[rows:], imag[:rows] + real[rows:]
        cos, sin = w_ref[0, 0, :, at], w_ref[0, 1, :, at]
        l_ref[0, :rows, at], l_ref[1, :rows, at] = split(re * cos - im * sin)
        l_ref[0, rows:, at], l_ref[1, rows:, at] = split(re * sin + im * cos)
        return 0

    def second(j, _):
        at = column(j)
        value = (l_ref[0], l_ref[1])
        by_cos = dot3(value, (t_ref[0, 0, :, at], t_ref[0, 1, :, at]))
        by_sin = dot3(value, (t_ref[1, 0, :, at], t_ref[1, 1, :, at]))
        shape = (rows // ROWS, ROWS, tile)
        o_ref[:, 0, 0, :, at] = (by_cos[:rows] - by_sin[rows:]).reshape(shape)
        o_ref[:, 0, 1, :, at] = (by_sin[:rows] + by_cos[rows:]).reshape(shape)
        return 0

    lax.fori_loop(0, low // tile, first, 0)
    lax.fori_loop(0, low // tile, second, 0)


def inverse_kernel(tile, own, units, final, x_ref, m_ref, w_ref, t_ref, *rest):
    a_ref, o_ref, l_ref = rest if len(rest) == 3 else (None, *rest)
    high, low = m_ref.shape[2], t_ref.shape[3]
    rows = x_ref.shape[0] * ROWS
    lanes = tile // 128
    for part in range(2):
        value = split(x_ref[:, 0, part].reshape(rows, low))
        l_ref[0, part * rows:(part + 1) * rows], l_ref[1, part * rows:(part + 1) * rows] = value

    def column(j, _):
        at = pl.ds(pl.multiple_of(j * tile, tile), tile)
        value = (l_ref[0], l_ref[1])
        by_cos = dot3(value, (t_ref[0, 0, :, at], t_ref[0, 1, :, at]))
        by_sin = dot3(value, (t_ref[1, 0, :, at], t_ref[1, 1, :, at]))
        re, im = by_cos[:rows] + by_sin[rows:], by_cos[rows:] - by_sin[:rows]
        cos, sin = w_ref[0, 0, :, at], w_ref[0, 1, :, at]
        re, im = re * cos + im * sin, im * cos - re * sin
        m = (m_ref[0, 0], m_ref[0, 1])
        real = dot3(m, split(jnp.concatenate([re, im], axis=0)))
        imag = dot3(m, split(jnp.concatenate([im, -re], axis=0)))
        for part, value in enumerate((real, imag)):
            before = 0.0 if a_ref is None else a_ref[part, 0, :, at]
            if units > 1:
                before = jnp.where(pl.program_id(1) == 0, before, o_ref[part, 0, :, at])
            value = value + before
            if final:
                for i, (p, r) in enumerate(columns(o_ref, part, j * lanes, lanes, own, high)):
                    o_ref[p, r, :] = value[:, i * 128:(i + 1) * 128]
            else:
                o_ref[part, 0, :, at] = value
        return 0

    lax.fori_loop(0, low // tile, column, 0)


def rotate(value, step, period, scale=1.0):
    re, im = value
    step %= period
    if (4 * step) % period == 0:
        turns = (4 * step) // period
        re, im = [(re, im), (-im, re), (-re, -im), (im, -re)][turns]
        return (re, im) if scale == 1.0 else (re * scale, im * scale)
    angle = 2.0 * math.pi * step / period
    cos, sin = math.cos(angle) * scale, math.sin(angle) * scale
    if (8 * step) % period == 0:
        root = math.sqrt(0.5) * scale
        plus, minus = (re + im) * root, (re - im) * root
        return {1: (minus, plus), 3: (-plus, minus), 5: (-minus, -plus), 7: (plus, -minus)}[(8 * step) // period]
    return re * cos - im * sin, re * sin + im * cos


def add(a, b):
    return a[0] + b[0], a[1] + b[1]


def sub(a, b):
    return a[0] - b[0], a[1] - b[1]


def small_dft(values, sign):
    n = len(values)
    if n == 1:
        return values
    if n % 4:
        return [add(values[0], values[1]), sub(values[0], values[1])]
    q = n // 4
    parts = [[], [], [], []]
    for i in range(q):
        a, b, c, d = values[i], values[i + q], values[i + 2 * q], values[i + 3 * q]
        s, t, u, v = add(a, c), sub(a, c), add(b, d), rotate(sub(b, d), sign, 4)
        parts[0].append(add(s, u))
        parts[1].append(rotate(add(t, v), sign * i, n))
        parts[2].append(rotate(sub(s, u), 2 * sign * i, n))
        parts[3].append(rotate(sub(t, v), 3 * sign * i, n))
    done = [small_dft(part, sign) for part in parts]
    return [done[i % 4][i // 4] for i in range(n)]


def square_kernel(blocks, start, scale, x_ref, *rest):
    sign = (1 - 2 * ((start + pl.program_id(0)) % 2)).astype(jnp.float32)
    o_ref = rest[-1]
    owners, own = x_ref.shape[:2]
    count = owners * own
    half = count // 2
    period = 3 * half

    def place(q):
        eighth, block = divmod(q, blocks)
        return (eighth // own) * blocks + block, eighth % own

    def load(q):
        owner, e = place(q)
        return x_ref[owner, e, 0], x_ref[owner, e, 1]

    third = []
    for rho in range(3):
        folded = [
            rotate(add(load(q), rotate(load(q + half), rho, 3)), rho * q, period) for q in range(half)
        ]
        values = small_dft(folded, 1)
        values = [(re * re - im * im, 2.0 * (re * im)) for re, im in values]
        values = small_dft(values, -1)
        third.append([rotate(value, -rho * q, period) for q, value in enumerate(values)])

    def coefficient(c):
        q, s = c % half, c // half
        total = third[0][q]
        for rho in (1, 2):
            total = add(total, rotate(third[rho][q], -rho * s, 3))
        return total

    before = coefficient(half - 1)
    for c in range(half, 3 * half):
        now = coefficient(c)
        both = now[0] + sign * before[0], now[1] + sign * before[1]
        owner, e = place(c - half)
        o_ref[owner, e, 0] = both[0] * scale
        o_ref[owner, e, 1] = both[1] * scale
        before = now


def plan(own, width, devices, blocks):
    units = UNITS
    while units > 2 and width // (devices * ROWS * units // 2) < 128:
        units //= 2
    rows = devices * ROWS
    high = rows * units // 2
    low = width // high
    tile = min(TILE, low)

    highs, lows = np.arange(high), np.arange(low)
    low_tables = np.stack([host_split(table) for table in host_turn(lows, lows, low)])
    twiddles, befores, afters = [], [], []
    for unit in range(units):
        freq = 2 * (unit // 2 * rows + np.arange(rows)) + unit % 2
        twiddles.append(np.stack(host_turn(freq, lows, 2 * width)).astype(np.float32))
        cos, sin = host_turn(freq, highs, 2 * high)
        befores.append(host_split(np.concatenate([cos, sin], axis=0)))
        afters.append(host_split(np.concatenate([cos.T, sin.T], axis=1)))
    low_tables, twiddles, befores, afters = [
        jnp.asarray(a) for a in (low_tables, np.stack(twiddles), np.stack(befores), np.stack(afters))
    ]

    once = pl.Buffered(1)
    tables = pl.BlockSpec(low_tables.shape, lambda e, u: (0, 0, 0, 0), pipeline_mode=once)
    woven = (2, own * width // 128, 128)
    plain = (2, own, high, low)
    plains = pl.BlockSpec((2, 1, high, low), lambda e, u: (0, e, 0, 0))
    packet = pl.BlockSpec((devices, 1, 2, ROWS, low), lambda e, u: (0, e, 0, u, 0))
    params = pltpu.CompilerParams(vmem_limit_bytes=VMEM)
    sums = pltpu.VMEM((2, 2 * rows, low), jnp.bfloat16)

    def of_unit(start, table):
        return pl.BlockSpec((1, *table.shape[1:]), lambda e, u: (start + u, 0, 0, 0))

    def message(count):
        return jax.ShapeDtypeStruct((devices, own, 2, count * ROWS, low), jnp.float32)

    def cost(count):
        flops = count * own * 3 * 8 * rows * low * (high + low)
        return pl.CostEstimate(flops=flops, bytes_accessed=8 * own * width, transcendentals=0)

    def forward(start, count, modes):
        field = modes.reshape(2, own, width // 128, 128).transpose(0, 2, 1, 3).reshape(woven)
        return pl.pallas_call(
            functools.partial(forward_kernel, tile, own),
            out_shape=message(count),
            grid=(own, count),
            in_specs=[
                pl.BlockSpec(woven, lambda e, u: (0, 0, 0), pipeline_mode=once),
                of_unit(start, befores),
                of_unit(start, twiddles),
                tables,
            ],
            out_specs=packet,
            scratch_shapes=[pltpu.VMEM((2, 2, high, low), jnp.bfloat16), sums],
            compiler_params=params,
            cost_estimate=cost(count),
            name="forward",
        )(field, befores, twiddles, low_tables)

    def inverse(start, count, packets, total, final):
        extra = [] if total is None else [total]
        out = pl.pallas_call(
            functools.partial(inverse_kernel, tile, own, count, final),
            out_shape=jax.ShapeDtypeStruct(woven if final else plain, jnp.float32),
            grid=(own, count),
            in_specs=[packet, of_unit(start, afters), of_unit(start, twiddles), tables, *([plains] * len(extra))],
            out_specs=pl.BlockSpec(woven, lambda e, u: (0, 0, 0)) if final else plains,
            scratch_shapes=[sums],
            compiler_params=params,
            cost_estimate=cost(count),
            name="inverse",
        )(packets, afters, twiddles, low_tables, *extra)
        if not final:
            return out
        return out.reshape(2, width // 128, own, 128).transpose(0, 2, 1, 3).reshape(2, own, width)

    def square(start, skip, count, packets, into, offset, room):
        def lanes(first):
            return pl.BlockSpec((devices, own, 2, ROWS, 128), lambda u, j: (0, 0, 0, first + u, j))

        scale = 1.0 / (3 * devices * own * width)
        extra = [] if into is None else [into]
        return pl.pallas_call(
            functools.partial(square_kernel, blocks, start, scale),
            out_shape=message(room),
            grid=(count, low // 128),
            in_specs=[lanes(skip), *([pl.BlockSpec(memory_space=pl.ANY)] * len(extra))],
            out_specs=lanes(offset),
            input_output_aliases={1: 0} if extra else {},
            compiler_params=params,
            cost_estimate=cost(count),
            name="square",
        )(packets, *extra)

    return units, forward, square, inverse


def cuts(units):
    if units >= 8:
        return [0, units // 8, units // 2, units], [0, units // 2, units - 1, units]
    return [0, 1, units], sorted({0, 1, units - 1, units})


def on_device(modes):
    own, width = modes.shape[1:]
    blocks = lax.axis_size("blk")
    devices = blocks * lax.axis_size("res")
    units, forward, square, inverse = plan(own, width, devices, blocks)
    there, back = cuts(units)

    def exchange(packets):
        return lax.all_to_all(packets, AXES, split_axis=0, concat_axis=0, tiled=True)

    arrived = [(a, b, exchange(forward(a, b - a, modes))) for a, b in zip(there, there[1:])]
    homes, total = [], None
    for a, b in zip(back, back[1:]):
        packets = None
        for c, d, values in arrived:
            start, end = max(a, c), min(b, d)
            if start < end:
                packets = square(start, start - c, end - start, values, packets, start - a, b - a)
        if len(homes) >= 2:
            total = inverse(*homes[-2], total, False)
            packets, total = lax.optimization_barrier((packets, total))
        homes.append((a, b - a, exchange(packets)))
    total = inverse(*homes[-2], total, False)
    return inverse(*homes[-1], total, True)


def solution(mesh):
    return jax.shard_map(
        on_device,
        mesh=mesh,
        in_specs=(P(None, "res", "blk"),),
        out_specs=P(None, "res", "blk"),
        check_vma=False,
    )
```
